32 devices in a mesh: row: 4 (over z), col: 8 (over y, x, core).
Axes of the slice: x: 2, y: 2, z: 4, core: 2. Of those that a mesh axis runs over, the one named last changes fastest.
Arguments:
- tokens: bfloat16 [3072, 8192], P(('row', 'col')), may hold values from -6 to 6
- up_weight: bfloat16 [8192, 14336], P('row', 'col'), may hold values from -0.0625 to 0.0625
Outputs:
- projected: bfloat16 [3072, 14336], P('row', 'col')
The draws below stay inside these ranges and needn't reach their ends.
All inputs are finite; a program needn't handle non-finite values.
Results may differ from the reference program's by a relative error of at most 0.001.
Values may be sent and summed in bfloat16 or wider, within the bound.
A program may use at most 128 MiB of HBM per device.

```python
import jax
import jax.numpy as jnp

D = 8192
FF = 14336
TOKENS = 3072


def block_levels(stream_key, shape, pieces, least, high):
    gain = 1.0
    for axis_at, blocks in pieces:
        heights = jax.random.uniform(jax.random.fold_in(jax.random.fold_in(stream_key, 6), axis_at), (blocks,), jnp.float32, least / len(pieces), high / len(pieces))
        gain = gain * jnp.repeat(jnp.exp(heights), shape[axis_at] // blocks).reshape((-1,) + (1,) * (len(shape) - 1 - axis_at))
    return gain


def scatter_about(stream_key, extent, scale, bound, pieces=(), held_as=jnp.bfloat16):
    array = jax.random.normal(stream_key, extent, jnp.float32) * scale
    if len(pieces) > 0:
        array = block_levels(stream_key, extent, pieces, -0.22, 0.18) * array
    return jnp.clip(array, min=-bound, max=bound).astype(held_as)


def setup_inputs(seed: int = 0) -> dict:
    arg_keys = jax.random.split(jax.random.key(seed), 3)
    return {
        "tokens": scatter_about(arg_keys[0], (TOKENS, D), 1.0, 6.0, ((0, 32),)),
        "up_weight": scatter_about(arg_keys[1], (D, FF), D ** -0.5, 0.0625, ((0, 4), (1, 8))),
    }


def reference(tokens, up_weight):
    sums = jnp.dot(tokens.astype(jnp.float32), up_weight.astype(jnp.float32), preferred_element_type=jnp.float32)
    return sums.astype(jnp.bfloat16)
```

```python
import jax
import jax.numpy as jnp
from jax import lax
from jax.sharding import PartitionSpec as P

LINE = 4
PIECES = 4


def column_pieces(columns):
    unit = 256 if columns % 256 == 0 else 128 if columns % 128 == 0 else 1
    units = columns // unit
    pieces = min(PIECES, units)
    edges = [unit * (units * i // pieces) for i in range(pieces + 1)]
    return list(zip(edges[:-1], edges[1:]))


def dot32(a, b):
    return jnp.dot(a, b, preferred_element_type=jnp.float32)


def gathered_weights(tokens, up_weight):
    w_column = lax.all_gather(up_weight, "row", axis=0, tiled=True)
    return dot32(lax.all_gather(tokens, "col", axis=0, tiled=True), w_column).astype(jnp.bfloat16)


def on_line(tokens, up_weight):
    z = lax.axis_index("row")
    depth, columns = up_weight.shape
    half = 2 * depth
    upper = z // 2
    inward, across, outward = [(0, 1), (3, 2)], [(1, 2), (2, 1)], [(1, 0), (2, 3)]
    outer = (z == 0) | (z == 3)

    def of_half(a, h):
        return lax.dynamic_slice_in_dim(a, h * half, half, axis=1)

    def gather(a):
        return lax.all_gather(a, "col", axis=0, tiled=True)

    outer_tokens = lax.ppermute(tokens, "row", inward)
    other_self = lax.ppermute(of_half(tokens, 1 - upper), "row", across)
    other_outer = lax.ppermute(of_half(outer_tokens, 1 - upper), "row", across)
    mine_self, mine_outer = of_half(tokens, upper), of_half(outer_tokens, upper)

    pieces = column_pieces(columns)
    w_own = [up_weight[:, a:b] for a, b in pieces]
    w_far = [lax.ppermute(w, "row", inward) for w in w_own]
    w_all = []
    for own, far in zip(w_own, w_far):
        low, high = lax.select(upper == 0, far, own), lax.select(upper == 0, own, far)
        w_all.append(jnp.concatenate([low, high], axis=0))

    rows_other_self = gather(other_self)
    rows_other_outer = gather(other_outer)
    rows_mine_outer = gather(mine_outer)
    rows_mine_self = gather(mine_self)

    result = []
    sums_self = [lax.ppermute(dot32(rows_other_self, w), "row", across) for w in w_all]
    sums_outer = [lax.ppermute(dot32(rows_other_outer, w), "row", across) for w in w_all]
    for w, s_self, s_outer in zip(w_all, sums_self, sums_outer):
        out_outer = (dot32(rows_mine_outer, w) + s_outer).astype(jnp.bfloat16)
        out_self = (dot32(rows_mine_self, w) + s_self).astype(jnp.bfloat16)
        from_inner = lax.ppermute(out_outer, "row", outward)
        result.append(lax.select(outer, from_inner, out_self))
    return jnp.concatenate(result, axis=1)


def solution(mesh):
    on_device = on_line if mesh.shape["row"] == LINE else gathered_weights
    in_specs = (P(("row", "col"), None), P("row", "col"))
    out_specs = P("row", "col")
    return jax.shard_map(
        on_device, mesh=mesh, in_specs=in_specs, out_specs=out_specs, check_vma=False
    )
```

```python
import jax
import jax.numpy as jnp
from jax import lax
from jax.sharding import PartitionSpec as P


LINE = 4
PIECES = 4


def column_pieces(columns):
    unit = 256 if columns % 256 == 0 else 128 if columns % 128 == 0 else 1
    units = columns // unit
    pieces = min(PIECES, units)
    edges = [unit * (-(-units * i // pieces)) for i in range(pieces + 1)]
    return list(zip(edges[:-1], edges[1:]))


def dot32(a, b):
    return jnp.dot(a, b, preferred_element_type=jnp.float32)


def gathered_weights(tokens, up_weight):
    w_column = lax.all_gather(up_weight, "row", axis=0, tiled=True)
    return dot32(lax.all_gather(tokens, "col", axis=0, tiled=True), w_column).astype(jnp.bfloat16)


def after(value, *others):
    return lax.optimization_barrier((value,) + others)[0]


def named_permute(value, pairs):
    return lax.ppermute(value, "row", pairs)


def on_line(tokens, up_weight):
    return line_plan(tokens, up_weight)


def middle_order(pieces):
    early, late = range(min(2, pieces)), range(min(2, pieces), pieces)
    return [("self", j) for j in early] + [("outer", j) for j in range(pieces)] + [("self", j) for j in late]


def line_plan(tokens, up_weight):
    z = lax.axis_index("row")
    depth, columns = up_weight.shape
    half = 2 * depth
    upper = z // 2
    inward, across, outward = [(0, 1), (3, 2)], [(1, 2), (2, 1)], [(1, 0), (2, 3)]
    outer = (z == 0) | (z == 3)

    def of_half(a, h):
        return lax.dynamic_slice_in_dim(a, h * half, half, axis=1)

    def gather(a):
        return lax.all_gather(a, "col", axis=0, tiled=True)

    pieces = column_pieces(columns)
    other_self = named_permute(of_half(tokens, 1 - upper), across)
    w_own = [up_weight[:, a:b] for a, b in pieces]
    w_far = [named_permute(w, inward) for w in w_own]
    outer_tokens = named_permute(tokens, inward)
    sent_outer, kept_outer = of_half(outer_tokens, 1 - upper), of_half(outer_tokens, upper)
    other_outer = named_permute(sent_outer, across)

    theirs, mine = {}, {}
    theirs["self"] = gather(other_self)
    mine["self"] = gather(after(of_half(tokens, upper), other_self))
    theirs["outer"] = gather(other_outer)
    mine["outer"] = gather(after(kept_outer, other_outer))

    weights = {}

    def weight(j, last):
        if j not in weights:
            own, far = w_own[j], w_far[j] if last is None else after(w_far[j], last)
            low, high = lax.select(upper == 0, far, own), lax.select(upper == 0, own, far)
            weights[j] = jnp.concatenate([low, high], axis=0)
        return weights[j]

    order = middle_order(len(pieces))
    last, sums = None, {}
    for kind, j in order:
        w = weight(j, last)
        rows = theirs[kind] if last is None else after(theirs[kind], last)
        last = dot32(rows, w)
        sums[kind, j] = named_permute(last, across)

    done = {}
    for kind, j in order:
        rows, arrived = after(mine[kind], last), after(sums[kind, j], last)
        last = (dot32(rows, weights[j]) + arrived).astype(jnp.bfloat16)
        done[kind, j] = named_permute(last, outward) if kind == "outer" else last
    result = [lax.select(outer, done["outer", j], done["self", j]) for j in range(len(pieces))]
    return jnp.concatenate(result, axis=1)


def solution(mesh):
    in_specs = (P(("row", "col"), None), P("row", "col"))
    out_specs = P("row", "col")

    def mapped(on_device):
        return jax.shard_map(
            on_device, mesh=mesh, in_specs=in_specs, out_specs=out_specs, check_vma=False
        )

    if mesh.shape["row"] != LINE:
        return mapped(gathered_weights)
    return mapped(on_line)
```
